128 devices in a mesh: gx: 8 (over x, core), gy: 16 (over z, y).
Axes of the slice: x: 4, y: 4, z: 4, core: 2. Of those that a mesh axis runs over, the one named last changes fastest.
Arguments:
- record_keys: int32 [131072], P(('gx', 'gy')), may hold values from 0 to 16777215
- payloads: int32 [131072], P(('gx', 'gy')), may hold values from 0 to 16777215
Outputs:
- sorted_keys: int32 [245760], P(('gx', 'gy'))
- sorted_payloads: int32 [245760], P(('gx', 'gy'))
- bucket_sizes: int32 [128], P(('gx', 'gy'))
- bucket_digest: int32 [128], P(('gx', 'gy'))
The draws below stay inside these ranges and needn't reach their ends.
All inputs are finite; a program needn't handle non-finite values.
Results may differ from the reference program's by a relative error of at most 0.000001.
Values may be sent and summed in bfloat16 or wider, within the bound.
A program may use at most 64 MiB of HBM per device.

```python
import math
import jax
import jax.numpy as jnp
import numpy as np
from jax import lax

KEYS_DEV = 1024
KEY_RANGE = 16777216
BUCKETS = 128
TOTAL = 131072
GROUP = 8
BUCKET_CAP = 1920


def plant(array, key, least, top_value):
    place = [jax.random.randint(jax.random.fold_in(key, axis), (), 0, length) for axis, length in enumerate(array.shape)]
    main_axis = array.shape.index(max(array.shape))
    neighbour = place[:main_axis] + [(place[main_axis] + 1) % array.shape[main_axis]] + place[main_axis + 1:]
    return array.at[tuple(place)].set(least).at[tuple(neighbour)].set(top_value)


def ranked_wide(rng, dims, amount, lean):
    portions = [min(1 << octave, amount + 1 - (1 << octave)) * (1 << 20) // math.isqrt((1 << octave) ** lean) + 1 for octave in range((amount + 1).bit_length()) if 1 << octave <= amount]
    deviation = 1 + sum(portions) // (1 << 30)
    listing = np.cumsum(np.array([max(1, weight // deviation) for weight in portions]))
    pick = jax.random.randint(jax.random.fold_in(rng, 1), dims, 0, int(listing[len(portions) - 1]))
    start = jnp.left_shift(1, jnp.searchsorted(jnp.asarray(listing, jnp.int32), pick, side="right").astype(jnp.int32))
    standing = start - 1 + jax.random.randint(jax.random.fold_in(rng, 4), dims, 0, 1 << 30) % jnp.minimum(start, amount + 1 - start)
    return jax.random.permutation(jax.random.fold_in(rng, 2), amount)[standing].astype(jnp.int32)


def setup_inputs(seed: int = 0) -> dict:
    seeds = jax.random.split(jax.random.key(seed), 3)
    return {
        "record_keys": plant(ranked_wide(seeds[0], (TOTAL,), KEY_RANGE, 2), jax.random.fold_in(seeds[0], 3), 0, KEY_RANGE - 1).astype(jnp.int32),
        "payloads": plant(jax.random.randint(seeds[1], (TOTAL,), 0, KEY_RANGE), jax.random.fold_in(seeds[1], 1), 0, KEY_RANGE - 1).astype(jnp.int32),
    }


def reference(record_keys, payloads):
    places = lax.iota(jnp.int32, TOTAL)
    block_keys, block_places = lax.sort(
        (record_keys.reshape(BUCKETS, KEYS_DEV), places.reshape(BUCKETS, KEYS_DEV)),
        dimension=1, num_keys=2)
    sample_keys = block_keys.reshape(BUCKETS, BUCKETS, GROUP)[:, :, GROUP - 1].reshape(-1)
    sample_places = block_places.reshape(BUCKETS, BUCKETS, GROUP)[:, :, GROUP - 1].reshape(-1)
    sample_keys, sample_places = lax.sort((sample_keys, sample_places), num_keys=2)
    split_places = sample_places.reshape(BUCKETS, BUCKETS)[:BUCKETS - 1, BUCKETS - 1]
    order_keys, order_places, order_values = lax.sort((record_keys, places, payloads), num_keys=2)
    rank_of = lax.sort((order_places, places), num_keys=1)[1]
    split_ranks = rank_of[split_places].astype(jnp.int32)
    begins = jnp.concatenate([jnp.zeros((1,), jnp.int32), split_ranks + 1])
    stop_at = jnp.concatenate([split_ranks + 1, jnp.full((1,), TOTAL, jnp.int32)])
    lengths = stop_at - begins
    offsets = lax.iota(jnp.int32, BUCKET_CAP)
    take_at = jnp.minimum(begins[:, None] + offsets[None, :], TOTAL - 1)
    filled = offsets[None, :] < lengths[:, None]
    grid_keys = jnp.where(filled, order_keys[take_at], -1)
    grid_values = jnp.where(filled, order_values[take_at], -1)
    mixed = (grid_keys + 3 * grid_values + 5 * offsets[None, :]) % 1024
    digest = jnp.sum(jnp.where(filled, 2 * mixed - 1023, 0), axis=1).astype(jnp.int32)
    return grid_keys.reshape(-1), grid_values.reshape(-1), lengths, digest
```

```python
import jax
import jax.numpy as jnp
from jax import lax
from jax.experimental import pallas as pl
from jax.experimental.pallas import tpu as pltpu
from jax.sharding import PartitionSpec as P

filler = 1 << 30
MESH = pl.DeviceIdType.MESH
f32, bf16, i32 = jnp.float32, jnp.bfloat16, jnp.int32


def iota(shape, dim):
    return lax.broadcasted_iota(i32, shape, dim)


def pieces(x):
    return [(x & 255).astype(f32), ((x >> 8) & 255).astype(f32), (x >> 16).astype(f32)]


def joined(p):
    p = [a.astype(i32) for a in p]
    return p[0] + (p[1] << 8) + (p[2] << 16)


def ranks_of(keys, n):
    across = jnp.transpose(keys)
    columns = [
        jnp.broadcast_to(across[:, a : a + 1], (128, 128)).reshape(16, 8, 128) for a in range(n)
    ]
    earlier = (iota((128, 128), 0) < iota((128, 128), 1)).astype(i32).reshape(16, 8, 128)
    ranks = []
    for e in range(n):
        row = keys[e : e + 1, :]
        total = jnp.zeros((8, 128), i32)
        for a in range(n):
            if a < e:
                below = columns[a] <= row
            elif a > e:
                below = columns[a] < row
            else:
                below = columns[a] < row + earlier
            total = total + jnp.sum(below.astype(i32), axis=0)
        ranks.append(jnp.sum(total, axis=0, keepdims=True))
    return ranks


def scattered(ranks, parts, rows):
    left, right = [], []
    high, low = iota((rows, 128), 0), iota((128, 128), 0)
    for rank, part in zip(ranks, parts):
        mine = (rank >> 7) == high
        left.append(
            jnp.concatenate([jnp.where(mine, p, 0.0) for p in part], axis=0).astype(bf16)
        )
        right.append(((rank & 127) == low).astype(f32).astype(bf16))
    left = jnp.concatenate(left, axis=1)
    right = jnp.concatenate(right, axis=1)
    return lax.dot_general(
        left, right, (((1,), (1,)), ((), ())), preferred_element_type=f32
    )


def sort_kernel(keys_ref, values_ref, out_ref):
    keys, values = keys_ref[...], values_ref[...]
    ranks = ranks_of(keys, 8)
    kp, vp = pieces(keys), pieces(values)
    parts = [[p[e : e + 1, :] for p in kp + vp] for e in range(8)]
    got = scattered(ranks, parts, 8)
    out_ref[0:8, :] = joined([got[8 * p : 8 * p + 8] for p in range(3)])
    out_ref[8:16, :] = joined([got[8 * p : 8 * p + 8] for p in range(3, 6)])


def place():
    gx, gy = lax.axis_index("gx"), lax.axis_index("gy")
    return gx, gy


def gather_kernel(run_ref, all_ref, send_sem, recv_sem, pair_send, pair_recv, own_sem):
    gx, gy = place()
    x, core = gx // 2, gx % 2
    z, y = gy // 4, gy % 4
    me = gx * 16 + gy
    own = pltpu.make_async_copy(run_ref, all_ref.at[me], own_sem)
    own.start()
    barrier = pltpu.get_barrier_semaphore()
    xs = [(x + d) % 4 for d in range(4)]
    ys = [(y + d) % 4 for d in range(4)]
    zs = [(z + d) % 4 for d in range(4)]
    peers = []
    for far in (6, 5, 4, 3, 2, 1):
        for dx in range(4):
            for dz in range(4):
                for dy in range(4):
                    if min(dx, 4 - dx) + min(dy, 4 - dy) + min(dz, 4 - dz) == far:
                        peers.append((xs[dx] * 2 + core, zs[dz] * 4 + ys[dy]))
    partner = (x * 2 + 1 - core, gy)
    for p in peers:
        pl.semaphore_signal(barrier, inc=1, device_id=p, device_id_type=MESH)
    pl.semaphore_signal(barrier, inc=1, device_id=partner, device_id_type=MESH)
    pl.semaphore_wait(barrier, 64)
    for p in peers:
        pltpu.make_async_remote_copy(
            src_ref=run_ref, dst_ref=all_ref.at[me], send_sem=send_sem, recv_sem=recv_sem,
            device_id=p, device_id_type=MESH,
        ).start()
    own.wait()
    many = all_ref.at[pl.ds(0, 63)]
    pltpu.make_async_copy(many, many, recv_sem).wait()
    for g in range(4):
        block = all_ref.at[pl.ds((2 * g + core) * 16, 16)]
        pltpu.make_async_remote_copy(
            src_ref=block, dst_ref=block, send_sem=pair_send, recv_sem=pair_recv,
            device_id=partner, device_id_type=MESH,
        ).start()
    half = all_ref.at[pl.ds(0, 64)]
    pltpu.make_async_copy(many, many, send_sem).wait()
    pltpu.make_async_copy(half, half, pair_send).wait()
    pltpu.make_async_copy(half, half, pair_recv).wait()


def merge_kernel(all_ref, keys_ref, values_ref, size_ref, digest_ref, comp_ref):
    gx, gy = place()
    me = gx * 16 + gy

    def chunk(r, c, which):
        return all_ref[pl.ds(128 * r + 8 * which + c, 8, stride=16), :]

    lane = iota((8, 128), 1)
    sample_at = (8 * lane + 7) & 127
    sample_chunk = lane >> 4
    samples = []
    for r in range(16):
        s = jnp.zeros((8, 128), i32)
        for c in range(8):
            v = jnp.take_along_axis(chunk(r, c, 0), sample_at, axis=1)
            s = jnp.where(sample_chunk == c, v, s)
        samples.append(s)
    samples = jnp.concatenate(samples, axis=0)
    samples3 = samples.reshape(16, 8, 128)

    targets = [(me * 128 - 1).astype(f32), (me * 128 + 127).astype(f32)]
    bases = [jnp.zeros((1, 128), i32)] * 2
    for bit in range(21, -1, -3):
        counts = []
        for base in bases:
            rows = []
            for d in range(8):
                least = base + (d << bit)
                c = jnp.sum((samples3 < least).astype(i32), axis=0)
                rows.append(jnp.sum(c, axis=0, keepdims=True))
            counts.append(jnp.concatenate(rows, axis=0).astype(f32))
        for s in range(2):
            total = jnp.broadcast_to(jnp.sum(counts[s], axis=1, keepdims=True), (8, 128))
            fits = (total <= targets[s]).astype(i32)
            digit = jnp.sum(fits, axis=0, keepdims=True) - 1
            bases[s] = bases[s] + (digit << bit)

    ones = jnp.ones((128, 128), bf16)
    lower = (iota((128, 128), 1) < iota((128, 128), 0)).astype(f32).astype(bf16)

    def dot(a, b):
        return jnp.dot(a, b, preferred_element_type=f32)

    def mask16(m):
        return m.astype(f32).astype(bf16)

    bounds = []
    for s in range(2):
        base, target = bases[s], targets[s]
        equal = dot(mask16(samples == base), ones)
        under = dot(mask16(samples < base), ones)
        before = dot(lower, equal.astype(bf16))
        rest = target - jnp.sum(under, axis=0, keepdims=True)
        past = before > rest
        whole = before + equal <= rest
        least = jnp.where(whole, base + 1, base)
        tallies = []
        for r in range(16):
            limit = least[8 * r : 8 * r + 8, :]
            t = jnp.zeros((8, 128), i32)
            for c in range(8):
                t = t + (chunk(r, c, 0) < limit).astype(i32)
            tallies.append(t)
        tally = jnp.concatenate(tallies, axis=0).astype(f32).astype(bf16)
        count = dot(tally, ones)
        cut = 8.0 * (under + rest - before) + 8.0
        bounds.append(jnp.where(past | whole, count, cut).astype(i32))
    begin = jnp.where(me == 0, 0, bounds[0])
    stop = jnp.where(me == 127, 1024, bounds[1])
    length = stop - begin
    coarse = (length >> 3).astype(f32)
    fine = (length & 7).astype(f32)
    offset = (
        8.0 * dot(lower, coarse.astype(bf16)) + dot(lower, fine.astype(bf16))
    ).astype(i32)
    upper = iota((128, 128), 0) < iota((128, 128), 1)
    ones16 = jnp.ones((16, 128), bf16)
    offset_row = (
        8.0 * dot(ones16, jnp.where(upper, coarse, 0.0).astype(bf16))
        + dot(ones16, jnp.where(upper, fine, 0.0).astype(bf16))
    ).astype(i32)
    size = jnp.sum(length, axis=0, keepdims=True)
    longest = jnp.max(length)

    def window(k):
        left = []
        high = iota((16, 128), 0)
        for carry in range(2):
            left.append(mask16((offset_row >> 7) + (k + carry) == high))
        left = jnp.concatenate(left, axis=1)
        first, second = [], []
        for r in range(16):
            b = begin[8 * r : 8 * r + 8, :]
            o = offset[8 * r : 8 * r + 8, :] & 127
            n = length[8 * r : 8 * r + 8, :] - 128 * k
            inner = b & 127
            at = (b >> 7) + k + (lane < inner).astype(i32)
            turn = (inner - o + lane) & 127
            valid = ((lane - o) & 127) < n
            here = valid & (lane >= o)
            over = valid & (lane < o)
            row1, row2 = [], []
            for which in range(2):
                v = chunk(r, 0, which)
                for c in range(1, 8):
                    v = jnp.where(at == c, chunk(r, c, which), v)
                v = jnp.take_along_axis(v, turn, axis=1)
                row1 += pieces(jnp.where(here, v, 0))
                row2 += pieces(jnp.where(over, v, 0))
            first.append(jnp.concatenate(row1, axis=1))
            second.append(jnp.concatenate(row2, axis=1))
        right = jnp.concatenate(first + second, axis=0).astype(bf16)
        return dot(left, right)

    comp_ref[...] = window(0)

    def more(k, _):
        comp_ref[...] += window(k)
        return 0

    lax.fori_loop(1, (longest + 127) >> 7, more, 0)
    comp = comp_ref[...]
    parts = [comp[:, 128 * p : 128 * p + 128] for p in range(6)]
    slot = iota((16, 128), 0) * 128 + iota((16, 128), 1)
    filled = slot < size
    keys = jnp.where(filled, joined(parts[:3]), filler)

    def finish(n):
        ranks = ranks_of(keys, n)
        got = scattered(ranks, [[p[e : e + 1, :] for p in parts] for e in range(n)], 16)
        k = jnp.where(filled, joined([got[16 * p : 16 * p + 16] for p in range(3)]), -1)
        v = jnp.where(filled, joined([got[16 * p : 16 * p + 16] for p in range(3, 6)]), -1)
        keys_ref[...] = k[:15]
        values_ref[...] = v[:15]
        mixed = (k + 3 * v + 5 * slot) & 1023
        digest_ref[0] = jnp.sum(jnp.where(filled, 2 * mixed - 1023, 0))

    total = jnp.max(size)
    size_ref[0] = total

    @pl.when(total <= 1152)
    def _():
        finish(9)

    @pl.when((total > 1152) & (total <= 1280))
    def _():
        finish(10)

    @pl.when(total > 1280)
    def _():
        finish(15)


VM = pl.BlockSpec(memory_space=pltpu.VMEM)
SM = pl.BlockSpec(memory_space=pltpu.SMEM)


def sort_call(keys, values):
    return pl.pallas_call(
        sort_kernel, out_shape=jax.ShapeDtypeStruct((16, 128), i32),
        in_specs=[VM, VM], out_specs=VM, name="sort_block",
    )(keys, values)


def gather_call(run):
    return pl.pallas_call(
        gather_kernel, out_shape=jax.ShapeDtypeStruct((128, 16, 128), i32),
        in_specs=[pl.BlockSpec(memory_space=pl.ANY)], out_specs=VM, name="gather_runs",
        scratch_shapes=[pltpu.SemaphoreType.DMA] * 5,
        compiler_params=pltpu.CompilerParams(collective_id=0, has_side_effects=True),
    )(run)


def merge_call(everything):
    return pl.pallas_call(
        merge_kernel,
        out_shape=(
            jax.ShapeDtypeStruct((15, 128), i32),
            jax.ShapeDtypeStruct((15, 128), i32),
            jax.ShapeDtypeStruct((1,), i32),
            jax.ShapeDtypeStruct((1,), i32),
        ),
        in_specs=[VM], out_specs=(VM, VM, SM, SM), name="merge_bucket",
        scratch_shapes=[pltpu.VMEM((16, 768), f32)],
    )(everything)


def shards(record_keys, payloads):
    run = sort_call(record_keys.reshape(8, 128), payloads.reshape(8, 128))
    everything = gather_call(run)
    k, v, size, digest = merge_call(everything.reshape(2048, 128))
    return k.reshape(1920), v.reshape(1920), size, digest


def solution(mesh):
    spec = P(("gx", "gy"))
    return jax.shard_map(
        shards, mesh=mesh, in_specs=(spec, spec), out_specs=(spec,) * 4, check_vma=False
    )
```
